32 devices in a mesh: dp: 8 (over z, core), expert: 4 (over y, x).
Axes of the slice: x: 2, y: 2, z: 4, core: 2. Of those that a mesh axis runs over, the one named last changes fastest.
Arguments:
- mamba_in: bfloat16 [8, 256, 4096], P('dp'), may hold values from -6 to 6
- conv_state: bfloat16 [8, 3, 8192], P('dp', None, 'expert'), may hold values from -6 to 6
- in_weight: bfloat16 [4096, 8192], P('dp', 'expert'), may hold values from -0.09375 to 0.09375
- conv_kernel: float32 [4, 8192], P(None, 'expert'), may hold values from -3 to 3
- conv_bias: float32 [8192], P('expert'), may hold values from -1 to 1
- moe_in: bfloat16 [512, 4096], P('expert'), may hold values from -6 to 6
- router: bfloat16 [4096, 4], replicated, may hold values from -0.09375 to 0.09375
- expert_ids: int32 [512, 2], P('expert'), may hold values from 0 to 3, all different within a row; in each aligned block of 128 rows (0 to 127, 128 to 255, ...) at most 128 rows name the same one
- w_gate: bfloat16 [4, 4096, 12288], P('expert', None, 'dp'), may hold values from -0.09375 to 0.09375
- w_up: bfloat16 [4, 4096, 12288], P('expert', None, 'dp'), may hold values from -0.09375 to 0.09375
- w_down: bfloat16 [4, 12288, 4096], P('expert', 'dp'), may hold values from -0.078125 to 0.078125
Outputs:
- conv_out: bfloat16 [8, 256, 8192], P('dp', None, 'expert')
- moe_out: bfloat16 [512, 4096], P('expert', 'dp')
The draws below stay inside these ranges and needn't reach their ends.
Inputs may be any that keep to these rules, and one draw needn't show every extreme that they name: `expert_ids`: each row names two different experts; among the 128 rows of one index of expert no expert is named more than 128 times, a bound that some block reaches.
All inputs are finite; a program needn't handle non-finite values.
Results may differ from the reference program's by a relative error of at most 0.0049.
Values may be sent and summed in bfloat16 or wider, within the bound.
No kernel may reach another device: no remote copies, remote signals or barrier semaphores. Data moves between devices by JAX's collectives and lax.ppermute only.
A program may use at most 192 MiB of HBM per device.

```python
import math
import jax
import jax.numpy as jnp
import numpy as np
from jax import lax

D = 4096
CH = 8192
FF = 12288
KW = 4
TOK = 256
TOKM = 128
SEQS = 8
EXPERTS = 4
TOKENS_M = 512
CAP = 128
N_EXPERT = 4


def strengthened(array, rng, source, target, parts, factor):
    def block_of(position):
        return (jnp.arange(array.shape[position]) // (array.shape[position] // parts)).reshape((-1,) + (1,) * (array.ndim - 1 - position))

    near = jax.random.permutation(rng, parts)[block_of(target)]
    second = (block_of(target) + parts // 2) % parts
    return jnp.where((block_of(source) == near) | (block_of(source) == second), factor * array, array)


def block_scale(rng, shape, split, least, high):
    level, own = 1.0, jax.random.fold_in(rng, 6)
    for dim, parts in split:
        steps = jnp.exp(jax.random.uniform(jax.random.fold_in(own, dim), (parts,), jnp.float32, least / len(split), high / len(split)))
        level = level * jnp.repeat(steps, shape[dim] // parts).reshape([-1 if axis == dim else 1 for axis in range(len(shape))])
    return level


def shared_out(own_key, own, number, rows, number_of, top, bound, skew):
    order = jax.random.permutation(own_key, number_of)
    packed, common = portions_of(number_of, rows * top, bound, skew, True), portions_of(number_of, rows * top, bound, skew, False)
    places = jnp.arange(number_of)

    def named(tallies, offset_by):
        used = int((tallies > 0).sum())
        fixed = max(1, used // 4)
        shifted = fixed + (places - fixed + offset_by * (used - fixed)) % max(1, number_of - fixed)
        return jnp.zeros((number_of,), jnp.int32).at[order[jnp.where(places < fixed, places, shifted)]].set(jnp.asarray(tallies, jnp.int32))

    tallies = jnp.where(number % 4 == 0, named(packed, number // 4), named(common, number - number // 4 - 1))
    mixed = jax.random.permutation(jax.random.fold_in(own, 3), number_of)
    donor, sink = mixed[0:number_of // 2 * 2:2], mixed[1:number_of // 2 * 2:2]
    slack = jnp.minimum(tallies[donor] - 1, bound - tallies[sink]) // 2
    slack = jnp.where((donor == order[0]) | (sink == order[0]) | (tallies[sink] == 0), 0, jnp.maximum(slack, 0))
    shifted = jax.random.randint(jax.random.fold_in(own, 4), (number_of // 2,), 0, 1 << 20) % (slack + 1)
    tallies = tallies.at[donor].add(-shifted).at[sink].add(shifted)
    labels = jnp.searchsorted(jnp.cumsum(tallies), jnp.arange(rows * top), side="right").astype(jnp.int32)
    table = labels.reshape(top, rows).T
    table = table[jax.random.permutation(jax.random.fold_in(own, 1), rows)]
    offset_by = jax.random.randint(jax.random.fold_in(own, 2), (rows, 1), 0, top)
    return jnp.take_along_axis(table, (jnp.arange(top)[None, :] + offset_by) % top, axis=1)


def portions_of(number_of, total, limit, lean, full):
    loads = [(1 << 20) // math.isqrt(grade ** lean) + 1 for grade in range(1, number_of + 1)]
    largest = limit if full else min(limit, max(-(-total // number_of), total * loads[0] // sum(loads)))
    least = 1 if total - largest >= number_of - 1 else 0
    given, spare = [largest] + [least] * (number_of - 1), total - largest - least * (number_of - 1)
    while spare > 0:
        movable = [i for i in range(1, number_of) if given[i] < largest] or [i for i in range(1, number_of) if given[i] < limit]
        pool, budget = sum([loads[i] for i in movable]), spare
        for i in movable:
            extra = min(limit - given[i], max(1, budget * loads[i] // pool), spare)
            given[i] = given[i] + extra
            spare = spare - extra
    return np.array(given)


def bell_draw(stream_key, extent, width, reach, pieces=(), held_as=jnp.bfloat16):
    array = width * jax.random.normal(stream_key, extent, jnp.float32)
    if pieces:
        array = array * block_scale(stream_key, extent, pieces, -0.22, 0.18)
    return jnp.clip(array, -reach, reach).astype(held_as)


def heavy_noise(own_key, shape, scale, most, shards, heavy, kind=jnp.bfloat16):
    entries = scale * jax.random.normal(own_key, shape, jnp.float32)
    if shards:
        entries = entries * block_scale(own_key, shape, shards, -0.22, 0.18)
    return jnp.clip(strengthened(entries, jax.random.fold_in(own_key, 3), *heavy), -most, most).astype(kind)


def setup_inputs(seed: int = 0) -> dict:
    key_list = jax.random.split(jax.random.key(seed), 12)
    mamba_in = bell_draw(key_list[0], (SEQS, TOK, D), 1.0, 6.0, ((0, 8),))
    conv_state = bell_draw(key_list[1], (SEQS, KW - 1, CH), 1.0, 6.0, ((0, 8), (2, 4)))
    in_weight = bell_draw(key_list[2], (D, CH), D ** -0.5, 0.09375, ((0, 8), (1, 4)))
    conv_kernel = bell_draw(key_list[3], (KW, CH), 0.5, 3.0, ((1, 4),), jnp.float32)
    conv_bias = jnp.clip(jax.random.uniform(key_list[4], (CH,), jnp.float32, -1.0, 1.0) * block_scale(key_list[4], (CH,), ((0, 4),), -0.4, 0.0), -1.0, 1.0)
    moe_in = bell_draw(key_list[5], (TOKENS_M, D), 1.0, 6.0, ((0, 4),))
    router = bell_draw(key_list[6], (D, EXPERTS), D ** -0.5, 0.09375)
    expert_ids_keys = jax.random.split(jax.random.fold_in(key_list[7], 1), TOKENS_M // TOKM)
    expert_ids_turns = jax.random.permutation(jax.random.fold_in(key_list[7], 3), TOKENS_M // TOKM)
    expert_ids = jax.vmap(lambda own, number: shared_out(jax.random.fold_in(key_list[7], 2), own, number, TOKM, EXPERTS, 2, CAP, 2))(expert_ids_keys, expert_ids_turns).reshape((TOKENS_M, 2))
    w_gate = bell_draw(key_list[8], (EXPERTS, D, FF), D ** -0.5, 0.09375, ((0, 4), (2, 8)))
    w_up = bell_draw(key_list[9], (EXPERTS, D, FF), D ** -0.5, 0.09375, ((0, 4), (2, 8)))
    w_down = heavy_noise(key_list[10], (EXPERTS, FF, D), FF ** -0.5, 0.078125, ((0, 4), (1, 8)), (1, 2, 8, 2.0))
    return {"mamba_in": mamba_in, "conv_state": conv_state, "in_weight": in_weight, "conv_kernel": conv_kernel, "conv_bias": conv_bias, "moe_in": moe_in, "router": router, "expert_ids": expert_ids, "w_gate": w_gate, "w_up": w_up, "w_down": w_down}


def slot_numbers(expert_ids, blocks, experts):
    block_ids = expert_ids.reshape(blocks, -1)
    onehot_ids = (block_ids[:, :, None] == jnp.arange(experts, dtype=jnp.int32)[None, None, :]).astype(jnp.int32)
    earlier = jnp.cumsum(onehot_ids, axis=1) - onehot_ids
    return jnp.sum(earlier * onehot_ids, axis=2).reshape(expert_ids.shape).astype(jnp.int32)


def run_expert(operands):
    inputs, gate_mat, up_mat, down_mat = operands
    gate_val = jnp.dot(inputs, gate_mat, preferred_element_type=jnp.float32)
    up_val = jnp.dot(inputs, up_mat, preferred_element_type=jnp.float32)
    hidden = (jax.nn.silu(gate_val) * up_val).astype(jnp.bfloat16)
    return jnp.dot(hidden, down_mat, preferred_element_type=jnp.float32)


def reference(mamba_in, conv_state, in_weight, conv_kernel, conv_bias, moe_in, router, expert_ids, w_gate, w_up, w_down):
    flat_in = mamba_in.reshape(SEQS * TOK, D)
    projected = jnp.dot(flat_in, in_weight, preferred_element_type=jnp.float32).astype(jnp.bfloat16)
    projected = projected.reshape(SEQS, TOK, CH)
    padded = jnp.concatenate([conv_state, projected], axis=1)
    summed = jnp.zeros((SEQS, TOK, CH), jnp.float32) + conv_bias[None, None, :]
    for offset in range(KW):
        summed = summed + padded[:, offset:offset + TOK].astype(jnp.float32) * conv_kernel[offset][None, None, :]
    conv_out = jax.nn.silu(summed).astype(jnp.bfloat16)

    expert_ids = expert_ids.astype(jnp.int32)
    slots = slot_numbers(expert_ids, N_EXPERT, EXPERTS)
    source = (jnp.arange(TOKENS_M, dtype=jnp.int32) // TOKM)[:, None]
    row_index = (source * CAP + slots).astype(jnp.int32)
    buffers = jnp.zeros((EXPERTS, N_EXPERT * CAP, D), jnp.bfloat16)
    token_rows = jnp.broadcast_to(moe_in[:, None, :], (TOKENS_M, 2, D))
    buffers = buffers.at[expert_ids, row_index].set(token_rows)
    outputs = lax.map(run_expert, (buffers, w_gate, w_up, w_down))
    logits = jnp.dot(moe_in, router, preferred_element_type=jnp.float32)
    chosen = jnp.take_along_axis(logits, expert_ids, axis=1)
    first_weight = jax.nn.sigmoid(chosen[:, 0] - chosen[:, 1])
    weights = jnp.stack([first_weight, 1.0 - first_weight], axis=1)
    picked = outputs[expert_ids, row_index]
    mixed = jnp.sum(weights[:, :, None] * picked, axis=1)
    return conv_out, mixed.astype(jnp.bfloat16)
```

```python
import jax
import jax.numpy as jnp
from jax import lax
from jax.sharding import PartitionSpec as P

F32 = jnp.float32
BF16 = jnp.bfloat16


def xor_send(value, axis, mask):
    pairs = [(i, i ^ mask) for i in range(lax.axis_size(axis))]
    return lax.ppermute(value, axis, pairs)


def body(
    mamba_in,
    conv_state,
    in_weight,
    conv_kernel,
    conv_bias,
    moe_in,
    router,
    expert_ids,
    w_gate,
    w_up,
    w_down,
):
    tokens, width = mamba_in.shape[1:]
    depth, channels = in_weight.shape
    taps = conv_kernel.shape[0]
    dp = lax.axis_size("dp")
    owners = lax.axis_size("expert")
    half = dp // 2
    me = lax.axis_index("dp")
    mine = lax.axis_index("expert")
    core = me % 2
    side = me // half
    local = me % half

    moe_rows = moe_in.shape[0]
    split = width // 2
    part = lax.dynamic_slice(moe_in, (0, core * split), (moe_rows, split))
    blocks = [moe_in]
    for mask in range(1, owners):
        got = xor_send(part, "expert", mask)
        other = xor_send(got, "dp", 1)
        first = jnp.where(core == 0, got, other)
        second = jnp.where(core == 0, other, got)
        blocks.append(jnp.concatenate([first, second], axis=1))

    window = mamba_in[0]
    features = width // 2
    share = tokens // owners
    piece = lax.dynamic_slice(window, (mine * share, (1 - side) * features), (share, features))
    piece = xor_send(piece, "dp", half)
    pieces = [piece] + [xor_send(piece, "expert", mask) for mask in range(1, owners)]
    far = jnp.zeros((tokens, features), BF16)
    for mask, block in enumerate(pieces):
        far = lax.dynamic_update_slice(far, block, ((mine ^ mask) * share, 0))
    near = lax.dynamic_slice(window, (0, side * features), (tokens, features))
    both = jnp.concatenate([near, far], axis=0)
    operands = [
        lax.dynamic_slice(both, (0, (local ^ mask) * depth), (2 * tokens, depth))
        for mask in range(half)
    ]

    chunks = 4
    cols = channels // chunks
    outs = []
    for chunk in range(chunks):
        own = in_weight[:, chunk * cols : (chunk + 1) * cols]
        total = None
        for mask in range(0, half, 2):
            even = own if mask == 0 else xor_send(own, "dp", mask)
            odd = xor_send(even, "dp", 1)
            for offset, weight in enumerate((even, odd)):
                term = jnp.dot(operands[mask + offset], weight, preferred_element_type=F32)
                total = term if total is None else total + term
        back = xor_send(total[tokens:].astype(BF16), "dp", half)
        projected = (total[:tokens] + back.astype(F32)).astype(BF16)
        lanes = slice(chunk * cols, (chunk + 1) * cols)
        extended = jnp.concatenate([conv_state[0][:, lanes], projected], axis=0)
        summed = jnp.zeros((tokens, cols), F32) + conv_bias[None, lanes]
        for tap in range(taps):
            summed = (
                summed
                + extended[tap : tap + tokens].astype(F32) * conv_kernel[tap][None, lanes]
            )
        outs.append(jax.nn.silu(summed).astype(BF16))
    conv_out = jnp.concatenate(outs, axis=1)[None]

    logits = jnp.dot(moe_in, router, preferred_element_type=F32)
    hits = expert_ids[:, :, None] == jnp.arange(router.shape[1], dtype=jnp.int32)[None, None, :]
    chosen = jnp.sum(jnp.where(hits, logits[:, None, :], 0.0), axis=2)
    first_weight = jax.nn.sigmoid(chosen[:, 0] - chosen[:, 1])
    pair = jnp.stack([first_weight, 1.0 - first_weight], axis=1)
    table = jnp.sum(jnp.where(hits, pair[:, :, None], 0.0), axis=1).T
    scales = []
    for mask in range(owners):
        row = lax.dynamic_slice(table, (mine ^ mask, 0), (1, moe_rows))
        scales.append(row if mask == 0 else xor_send(row, "expert", mask))
    scale = jnp.concatenate(scales, axis=1).reshape(-1, 1)

    rows = jnp.concatenate(blocks, axis=0)
    gate = jnp.dot(rows, w_gate[0], preferred_element_type=F32)
    up = jnp.dot(rows, w_up[0], preferred_element_type=F32)
    hidden = (jax.nn.silu(gate) * up).astype(BF16)
    result = jnp.dot(hidden, w_down[0], preferred_element_type=F32) * scale

    final = width // dp
    result = result.reshape(-1, half, 2, final)
    send = lax.dynamic_index_in_dim(result, 1 - core, 2, keepdims=False)
    keep = lax.dynamic_index_in_dim(result, core, 2, keepdims=False)
    keep = keep + xor_send(send, "dp", 1)
    keep = keep.reshape(owners, moe_rows, half, final)
    mixed = keep[0]
    for mask in range(1, owners):
        mixed = mixed + xor_send(keep[mask].astype(BF16), "expert", mask).astype(F32)
    place = me // 2
    answer = lax.dynamic_index_in_dim(mixed, place, 1, keepdims=False)
    for mask in range(1, half):
        share_out = lax.dynamic_index_in_dim(mixed, place ^ mask, 1, keepdims=False)
        answer = answer + xor_send(share_out.astype(BF16), "dp", 2 * mask).astype(F32)
    return conv_out, answer.astype(BF16)


def solution(mesh):
    in_specs = (
        P("dp", None, None),
        P("dp", None, "expert"),
        P("dp", "expert"),
        P(None, "expert"),
        P("expert"),
        P("expert", None),
        P(),
        P("expert", None),
        P("expert", None, "dp"),
        P("expert", None, "dp"),
        P("expert", "dp", None),
    )
    out_specs = (P("dp", None, "expert"), P("expert", "dp"))
    return jax.shard_map(body, mesh=mesh, in_specs=in_specs, out_specs=out_specs, check_vma=False)
```

```python
import functools

import jax
import jax.numpy as jnp
from jax import lax
from jax.experimental import pallas as pl
from jax.experimental.pallas import tpu as pltpu
from jax.sharding import PartitionSpec as P

F32 = jnp.float32
BF16 = jnp.bfloat16
LANES = 128
VMEM = 56 << 20
SMEM_SPEC = pl.BlockSpec(memory_space=pltpu.SMEM)
CHUNKS = 2


def xor_send(value, mask):
    pairs = [(i, i ^ mask) for i in range(lax.axis_size("dp"))]
    return lax.ppermute(value, "dp", pairs)


def owner_send(value, mask):
    pairs = [(i, i ^ mask) for i in range(lax.axis_size("expert"))]
    return lax.ppermute(value, "expert", pairs)


def after(value, *earlier):
    return lax.optimization_barrier((value, *earlier))[0]


def dot(left, right):
    return jnp.dot(left, right, preferred_element_type=F32)


def dot_t(left, right):
    return lax.dot_general(left, right, (((1,), (1,)), ((), ())), preferred_element_type=F32)


def whole(array):
    return pl.BlockSpec(array.shape, lambda *_: (0,) * array.ndim)


def tile_of(size, tile):
    return tile if size % tile == 0 else size


def half_product_kernel(blocks, depth, pieces, where, window, *refs):
    fars, weights = refs[:pieces], refs[pieces : pieces + blocks]
    near_out, far_out, rows = refs[pieces + blocks :]
    tokens = window.shape[1]

    @pl.when(pl.program_id(0) == 0)
    def _():
        for mask in range(blocks):
            source = pl.ds(pl.multiple_of((where[0] ^ mask) * depth, LANES), depth)
            lanes = slice(mask * depth, (mask + 1) * depth)
            rows[:tokens, lanes] = window[0, :, source]
            first = tokens
            for far in fars:
                rows[first : first + far.shape[0], lanes] = far[:, source]
                first += far.shape[0]

    total = None
    for mask in range(blocks):
        term = dot(rows[:, mask * depth : (mask + 1) * depth], weights[mask][...])
        total = term if mask == 0 else total + term
    near_out[...] = total[:tokens]
    far_out[...] = total[tokens:].astype(BF16)


def half_product(where, window, fars, weights, offset, cols):
    tokens, features = window.shape[1], fars[0].shape[1]
    depth = weights[0].shape[0]
    tile = tile_of(cols, 512)
    base = offset // tile

    def spec(weight):
        first = base if weight.shape[1] != cols else 0
        return pl.BlockSpec((depth, tile), lambda i, where: (0, first + i))

    return pl.pallas_call(
        functools.partial(half_product_kernel, len(weights), depth, len(fars)),
        grid_spec=pltpu.PrefetchScalarGridSpec(
            num_scalar_prefetch=1,
            grid=(cols // tile,),
            in_specs=[pl.BlockSpec((1, tokens, features), lambda i, where: (0, 0, where[1]))]
            + [whole(far) for far in fars]
            + [spec(weight) for weight in weights],
            out_specs=[pl.BlockSpec((tokens, tile), lambda i, where: (0, i))] * 2,
            scratch_shapes=[pltpu.VMEM((2 * tokens, features), BF16)],
        ),
        out_shape=[
            jax.ShapeDtypeStruct((tokens, cols), F32),
            jax.ShapeDtypeStruct((tokens, cols), BF16),
        ],
        compiler_params=pltpu.CompilerParams(vmem_limit_bytes=VMEM),
        cost_estimate=pl.CostEstimate(
            flops=4 * tokens * features * cols,
            transcendentals=0,
            bytes_accessed=2 * features * (2 * tokens + cols) + 6 * tokens * cols,
        ),
        name="half_product",
    )(where, window, *fars, *weights)


def conv_kernel_body(pad, pieces, where, own, back, state, taps, bias, *refs):
    out, rows = refs[-2:]
    tokens = own.shape[0]
    count = taps.shape[0]
    rows[pad - (count - 1) : pad, :] = state[0].astype(F32)
    share = tokens // pieces
    for mask in range(pieces):
        start = pl.multiple_of((where[1] ^ mask) * share, 8)
        piece = back[mask * share : (mask + 1) * share, :].astype(F32)
        value = (own[pl.ds(start, share), :] + piece).astype(BF16).astype(F32)
        rows[pl.ds(pl.multiple_of(pad + start, 8), share), :] = value
    summed = bias[...]
    for tap in range(count):
        first = pad - (count - 1) + tap
        summed = summed + rows[first : first + tokens, :] * taps[tap : tap + 1, :]
    out[0] = jax.nn.silu(summed).astype(BF16)


def conv(where, pieces, own, back, state, taps, bias, offset, channels, earlier):
    tokens, cols = own.shape
    tile = tile_of(cols, 512)
    base = offset // tile
    count = taps.shape[0]
    pad = 8
    inputs = [where, own, back, state, taps, bias]
    in_specs = [
        SMEM_SPEC,
        pl.BlockSpec((tokens, tile), lambda i: (0, i)),
        pl.BlockSpec((tokens, tile), lambda i: (0, i)),
        pl.BlockSpec((1, count - 1, tile), lambda i: (0, 0, base + i)),
        pl.BlockSpec((count, tile), lambda i: (0, base + i)),
        pl.BlockSpec((1, tile), lambda i: (0, base + i)),
    ]
    aliases = {}
    if earlier is not None:
        inputs.append(earlier)
        in_specs.append(pl.BlockSpec(memory_space=pl.ANY))
        aliases = {6: 0}
    return pl.pallas_call(
        functools.partial(conv_kernel_body, pad, pieces),
        grid=(cols // tile,),
        in_specs=in_specs,
        out_specs=pl.BlockSpec((1, tokens, tile), lambda i: (0, 0, base + i)),
        out_shape=jax.ShapeDtypeStruct((1, tokens, channels), BF16),
        scratch_shapes=[pltpu.VMEM((pad + tokens, tile), F32)],
        input_output_aliases=aliases,
        compiler_params=pltpu.CompilerParams(vmem_limit_bytes=VMEM),
        cost_estimate=pl.CostEstimate(
            flops=12 * tokens * cols,
            transcendentals=tokens * cols,
            bytes_accessed=8 * tokens * cols,
        ),
        name="conv",
    )(*inputs)


def hidden_kernel(quarter, where, *refs):
    inputs, router, gates, ups = refs[:4], refs[4], refs[5:9], refs[9:13]
    hidden, scale = refs[13:]
    gated = raised = None
    for source, gate, up in zip(inputs, gates, ups):
        rows = source[:, :quarter]
        one, two = dot(rows, gate[0]), dot(rows, up[0])
        gated = one if gated is None else gated + one
        raised = two if raised is None else raised + two
    hidden[...] = (jax.nn.silu(gated) * raised).astype(BF16)

    @pl.when(pl.program_id(0) == 0)
    def _():
        core, owner = where[0], where[1]
        logits = None
        for number, source in enumerate(inputs):
            block = 2 * core + number if number < 2 else 2 * (1 - core) + number - 2
            lanes = pl.ds(pl.multiple_of(block * quarter, LANES), quarter)
            term = dot_t(source[:, :quarter], router[:, lanes])
            logits = term if logits is None else logits + term
        lane = lax.broadcasted_iota(jnp.int32, logits.shape, 1)
        ids = inputs[1][:, quarter:].astype(jnp.int32)
        ids_a, ids_b = ids[:, 0:1], ids[:, 1:2]
        chosen_a = jnp.sum(jnp.where(lane == ids_a, logits, 0.0), axis=1, keepdims=True)
        chosen_b = jnp.sum(jnp.where(lane == ids_b, logits, 0.0), axis=1, keepdims=True)
        weight = jax.nn.sigmoid(chosen_a - chosen_b)
        mixed = jnp.where(ids_a == owner, weight, 0.0) + jnp.where(
            ids_b == owner, 1.0 - weight, 0.0
        )
        scale[...] = jnp.broadcast_to(mixed, scale.shape)


def hidden_units(where, inputs, router, w_gate, w_up):
    rows, quarter = inputs[0].shape
    width, units = w_gate.shape[1:]
    tile = tile_of(units, 256)

    def spec(number):
        def place(i, where):
            return 0, 2 * where[0] + number if number < 2 else 2 - 2 * where[0] + number - 2, i

        return pl.BlockSpec((1, quarter, tile), place)

    specs = [spec(number) for number in range(4)]
    return pl.pallas_call(
        functools.partial(hidden_kernel, quarter),
        grid_spec=pltpu.PrefetchScalarGridSpec(
            num_scalar_prefetch=1,
            grid=(units // tile,),
            in_specs=[whole(array) for array in (*inputs, router)] + specs + specs,
            out_specs=[
                pl.BlockSpec((rows, tile), lambda i, where: (0, i)),
                pl.BlockSpec((rows, LANES), lambda i, where: (0, 0)),
            ],
        ),
        out_shape=[
            jax.ShapeDtypeStruct((rows, units), BF16),
            jax.ShapeDtypeStruct((rows, LANES), F32),
        ],
        compiler_params=pltpu.CompilerParams(vmem_limit_bytes=VMEM),
        cost_estimate=pl.CostEstimate(
            flops=4 * rows * width * units,
            transcendentals=rows * units,
            bytes_accessed=4 * width * units + 4 * rows * width,
        ),
        name="hidden_units",
    )(where, *inputs, router, *[w_gate] * 4, *[w_up] * 4)


def down_kernel(steps, where, hidden, scale, down, send, keep):
    value = dot(hidden[...], down[0]) * scale[:, 0:1]

    @pl.when(pl.program_id(0) < steps)
    def _():
        send[...] = value.astype(BF16)

    @pl.when(pl.program_id(0) >= steps)
    def _():
        keep[...] = value


def down_units(where, hidden, scale, w_down, final):
    rows, units = hidden.shape
    width = w_down.shape[2]
    steps = width // final // 2

    def place(i, where):
        parity = jnp.where(i < steps, 1 - where[0], where[0])
        return 0, 0, 2 * lax.rem(i, steps) + parity

    return pl.pallas_call(
        functools.partial(down_kernel, steps),
        grid_spec=pltpu.PrefetchScalarGridSpec(
            num_scalar_prefetch=1,
            grid=(2 * steps,),
            in_specs=[
                pl.BlockSpec(hidden.shape, lambda i, where: (0, 0)),
                pl.BlockSpec(scale.shape, lambda i, where: (0, 0)),
                pl.BlockSpec((1, units, final), place),
            ],
            out_specs=[
                pl.BlockSpec((rows, final), lambda i, where: (0, jnp.minimum(i, steps - 1))),
                pl.BlockSpec((rows, final), lambda i, where: (0, jnp.maximum(i - steps, 0))),
            ],
        ),
        out_shape=[
            jax.ShapeDtypeStruct((rows, width // 2), BF16),
            jax.ShapeDtypeStruct((rows, width // 2), F32),
        ],
        compiler_params=pltpu.CompilerParams(vmem_limit_bytes=VMEM),
        cost_estimate=pl.CostEstimate(
            flops=2 * rows * width * units,
            transcendentals=0,
            bytes_accessed=2 * width * units + 2 * rows * (units + width),
        ),
        name="down_units",
    )(where, hidden, scale, w_down)


def collect_kernel(places, final, where, *refs):
    count = len(refs) - places - 1
    sides, outs, rows = refs[:count], refs[count:-1], refs[-1]
    offset = 0
    for pair in range(0, count, 2):
        value = sides[pair][...] + sides[pair + 1][...].astype(F32)
        rows[:, offset : offset + value.shape[1]] = value
        offset += value.shape[1]
    for mask in range(places):
        start = pl.multiple_of((where[2] ^ mask) * final, LANES)
        value = rows[:, pl.ds(start, final)]
        outs[mask][...] = value if mask == 0 else value.astype(BF16)


def collect(where, sides, final, places):
    rows = sides[0].shape[0]
    vmem = pl.BlockSpec(memory_space=pltpu.VMEM)
    return pl.pallas_call(
        functools.partial(collect_kernel, places, final),
        in_specs=[SMEM_SPEC] + [vmem] * len(sides),
        out_specs=[vmem] * places,
        out_shape=[jax.ShapeDtypeStruct((rows, final), F32)]
        + [jax.ShapeDtypeStruct((rows, final), BF16)] * (places - 1),
        scratch_shapes=[pltpu.VMEM((rows, places * final), F32)],
        name="collect",
    )(where, *sides)


def body(
    mamba_in,
    conv_state,
    in_weight,
    conv_kernel,
    conv_bias,
    moe_in,
    router,
    expert_ids,
    w_gate,
    w_up,
    w_down,
):
    tokens, width = mamba_in.shape[1:]
    channels = in_weight.shape[1]
    dp = lax.axis_size("dp")
    owners = lax.axis_size("expert")
    half = dp // 2
    me = lax.axis_index("dp")
    mine = lax.axis_index("expert")
    core = me & 1
    side = jnp.where(me >= half, 1, 0)
    local = me & (half - 1)
    place = me >> 1
    final = width // dp
    moe_rows = moe_in.shape[0]
    split = width // 2
    quarter = split // 2
    features = width // 2
    share = tokens // owners
    cols = channels // CHUNKS
    where = jnp.stack([core, mine, place])
    spot = jnp.stack([local, side])
    columns = range(2, owners, 2)

    piece = lax.dynamic_slice(
        mamba_in, (0, mine * share, (1 - side) * features), (1, share, features)
    )[0]
    piece = xor_send(piece, half)

    left = lax.dynamic_slice(moe_in, (0, core * split), (moe_rows, quarter))
    right = lax.dynamic_slice(moe_in, (0, core * split + quarter), (moe_rows, quarter))
    names = jnp.pad(expert_ids.astype(BF16), ((0, 0), (0, LANES - expert_ids.shape[1])))
    right = jnp.concatenate([right, names], axis=1)
    lefts = {0: left, 1: owner_send(left, 1)}
    rights = {0: right}
    for mask in columns:
        rights[mask] = owner_send(right, mask)
    both = jnp.concatenate([lefts[0], lefts[1]], axis=0)
    for mask in columns:
        got = owner_send(both, mask)
        lefts[mask], lefts[mask + 1] = got[:moe_rows], got[moe_rows:]
    got = owner_send(jnp.concatenate([rights[mask] for mask in range(0, owners, 2)], axis=0), 1)
    for mask in range(0, owners, 2):
        rights[mask + 1] = got[mask // 2 * moe_rows : (mask // 2 + 1) * moe_rows]
    lefts = jnp.concatenate([lefts[mask] for mask in range(owners)], axis=0)
    rights = jnp.concatenate([rights[mask] for mask in range(owners)], axis=0)
    inputs = [lefts, rights, xor_send(lefts, 1), xor_send(rights[:, :quarter], 1)]

    fars = [piece, owner_send(piece, 1)]
    both = jnp.concatenate(fars, axis=0)
    for mask in columns:
        fars.append(owner_send(both, mask))

    paired = xor_send(in_weight, 1)
    weights, arrived = [], []
    for chunk in range(CHUNKS):
        block = in_weight[:, chunk * cols : (chunk + 1) * cols]
        entry, direct = [in_weight, paired], []
        for mask in range(2, half, 2):
            if chunk:
                block = after(block, *fars[1:])
            direct.append(xor_send(block, mask))
            entry += [direct[-1], xor_send(direct[-1], 1)]
        weights.append(entry)
        arrived.append(direct)

    def product(chunk, *earlier):
        own, out = half_product(
            spot, mamba_in, [after(fars[0], *earlier), *fars[1:]], weights[chunk], chunk * cols, cols
        )
        return own, out, xor_send(out, half)

    def convolve(chunk, own, come, before):
        return conv(
            where,
            owners,
            own,
            come,
            conv_state,
            conv_kernel,
            conv_bias[None],
            chunk * cols,
            channels,
            before,
        )

    inputs[0] = after(inputs[0], *fars, *arrived[0], paired)
    hidden, scale = hidden_units(where, inputs, router.T, w_gate, w_up)
    own_0, out_0, come_0 = product(0, hidden)
    hidden = after(hidden, out_0, *arrived[1])
    send, keep = down_units(where, hidden, scale, w_down, final)
    taken = xor_send(send, 1)
    own_1, out_1, come_1 = product(1, keep)
    taken = after(taken, out_1)
    total = (keep + taken.astype(F32)).reshape(owners, moe_rows, split)
    left, right = total[:, :, :quarter], total[:, :, quarter:]
    got = owner_send(jnp.concatenate([left[m] for m in range(1, owners, 2)], 0).astype(BF16), 1)
    got = got.reshape(owners // 2, moe_rows, quarter)
    left = {mask: left[mask] + got[mask // 2].astype(F32) for mask in range(0, owners, 2)}
    firsts, seconds = right[0], right[1]
    for mask in columns:
        got = owner_send(right[mask : mask + 2].reshape(-1, quarter).astype(BF16), mask)
        firsts = firsts + got[:moe_rows].astype(F32)
        seconds = seconds + got[moe_rows:].astype(F32)
    conv_out = convolve(0, after(own_0, firsts), come_0, None)
    lefts = left[0]
    for mask in columns:
        come = owner_send(left[mask].astype(BF16), mask)
        if mask != columns[-1]:
            lefts = lefts + come.astype(F32)
    sides = [lefts, come, firsts, owner_send(seconds.astype(BF16), 1)]
    answer, *outs = collect(where, sides, final, half)
    for mask, out in enumerate(outs, 1):
        answer = answer + xor_send(out, 2 * mask).astype(F32)
    conv_out = convolve(1, own_1, come_1, conv_out)
    return conv_out, answer.astype(BF16)


def solution(mesh):
    in_specs = (
        P("dp", None, None),
        P("dp", None, "expert"),
        P("dp", "expert"),
        P(None, "expert"),
        P("expert"),
        P("expert", None),
        P(),
        P("expert", None),
        P("expert", None, "dp"),
        P("expert", None, "dp"),
        P("expert", "dp", None),
    )
    out_specs = (P("dp", None, "expert"), P("expert", "dp"))
    return jax.shard_map(body, mesh=mesh, in_specs=in_specs, out_specs=out_specs, check_vma=False)
```

```python
import functools
import math

import jax
import jax.numpy as jnp
from jax import lax
from jax.experimental import pallas as pl
from jax.experimental.pallas import tpu as pltpu
from jax.sharding import PartitionSpec as P

F32 = jnp.float32
BF16 = jnp.bfloat16
LANES = 128
VMEM = 24 << 20
VMEM_ALL = 56 << 20
SMEM_SPEC = pl.BlockSpec(memory_space=pltpu.SMEM)
CHUNKS = (1, 1, 2)


def xor_send(value, mask):
    pairs = [(i, i ^ mask) for i in range(lax.axis_size("dp"))]
    return lax.ppermute(value, "dp", pairs)


def owner_send(value, mask):
    pairs = [(i, i ^ mask) for i in range(lax.axis_size("expert"))]
    return lax.ppermute(value, "expert", pairs)


def after(value, *earlier):
    return lax.optimization_barrier((value, *earlier))[0]


def dot(left, right):
    return jnp.dot(left, right, preferred_element_type=F32)


def dot_t(left, right):
    return lax.dot_general(left, right, (((1,), (1,)), ((), ())), preferred_element_type=F32)


def whole(array):
    return pl.BlockSpec(array.shape, lambda *_: (0,) * array.ndim)


def tile_of(size, tile):
    return tile if size % tile == 0 else size


def half_product_kernel(blocks, depth, pieces, where, window, *refs):
    fars, weights = refs[:pieces], refs[pieces : pieces + blocks]
    near_out, far_out, rows = refs[pieces + blocks :]
    tokens = window.shape[1]

    @pl.when(pl.program_id(0) == 0)
    def _():
        for mask in range(blocks):
            source = pl.ds(pl.multiple_of((where[0] ^ mask) * depth, LANES), depth)
            lanes = slice(mask * depth, (mask + 1) * depth)
            rows[:tokens, lanes] = window[0, :, source]
            first = tokens
            for far in fars:
                rows[first : first + far.shape[0], lanes] = far[:, source]
                first += far.shape[0]

    total = None
    for mask in range(blocks):
        term = dot(rows[:, mask * depth : (mask + 1) * depth], weights[mask][...])
        total = term if mask == 0 else total + term
    near_out[...] = total[:tokens]
    far_out[...] = total[tokens:].astype(BF16)


def half_product(where, window, fars, weights, offset, cols):
    tokens, features = window.shape[1], fars[0].shape[1]
    depth = weights[0].shape[0]
    tile = math.gcd(offset, cols, 512)
    base = offset // tile

    def spec(weight):
        first = base if weight.shape[1] != cols else 0
        return pl.BlockSpec((depth, tile), lambda i, where: (0, first + i))

    return pl.pallas_call(
        functools.partial(half_product_kernel, len(weights), depth, len(fars)),
        grid_spec=pltpu.PrefetchScalarGridSpec(
            num_scalar_prefetch=1,
            grid=(cols // tile,),
            in_specs=[pl.BlockSpec((1, tokens, features), lambda i, where: (0, 0, where[1]))]
            + [whole(far) for far in fars]
            + [spec(weight) for weight in weights],
            out_specs=[pl.BlockSpec((tokens, tile), lambda i, where: (0, i))] * 2,
            scratch_shapes=[pltpu.VMEM((2 * tokens, features), BF16)],
        ),
        out_shape=[
            jax.ShapeDtypeStruct((tokens, cols), F32),
            jax.ShapeDtypeStruct((tokens, cols), BF16),
        ],
        compiler_params=pltpu.CompilerParams(vmem_limit_bytes=VMEM),
        cost_estimate=pl.CostEstimate(
            flops=4 * tokens * features * cols,
            transcendentals=0,
            bytes_accessed=2 * features * (2 * tokens + cols) + 6 * tokens * cols,
        ),
        name="half_product",
    )(where, window, *fars, *weights)


def conv_kernel_body(pad, pieces, where, own, back, state, taps, bias, *refs):
    out, rows = refs[-2:]
    tokens = own.shape[0]
    count = taps.shape[0]
    rows[pad - (count - 1) : pad, :] = state[0].astype(F32)
    share = tokens // pieces
    for mask in range(pieces):
        start = pl.multiple_of((where[1] ^ mask) * share, 8)
        piece = back[mask * share : (mask + 1) * share, :].astype(F32)
        value = (own[pl.ds(start, share), :] + piece).astype(BF16).astype(F32)
        rows[pl.ds(pl.multiple_of(pad + start, 8), share), :] = value
    summed = bias[...]
    for tap in range(count):
        first = pad - (count - 1) + tap
        summed = summed + rows[first : first + tokens, :] * taps[tap : tap + 1, :]
    out[0] = jax.nn.silu(summed).astype(BF16)


def conv(where, pieces, own, back, state, taps, bias, offset, channels, earlier):
    tokens, cols = own.shape
    tile = math.gcd(offset, cols, 512)
    base = offset // tile
    count = taps.shape[0]
    pad = 8
    inputs = [where, own, back, state, taps, bias]
    in_specs = [
        SMEM_SPEC,
        pl.BlockSpec((tokens, tile), lambda i: (0, i)),
        pl.BlockSpec((tokens, tile), lambda i: (0, i)),
        pl.BlockSpec((1, count - 1, tile), lambda i: (0, 0, base + i)),
        pl.BlockSpec((count, tile), lambda i: (0, base + i)),
        pl.BlockSpec((1, tile), lambda i: (0, base + i)),
    ]
    aliases = {}
    if earlier is not None:
        inputs.append(earlier)
        in_specs.append(pl.BlockSpec(memory_space=pl.ANY))
        aliases = {6: 0}
    return pl.pallas_call(
        functools.partial(conv_kernel_body, pad, pieces),
        grid=(cols // tile,),
        in_specs=in_specs,
        out_specs=pl.BlockSpec((1, tokens, tile), lambda i: (0, 0, base + i)),
        out_shape=jax.ShapeDtypeStruct((1, tokens, channels), BF16),
        scratch_shapes=[pltpu.VMEM((pad + tokens, tile), F32)],
        input_output_aliases=aliases,
        compiler_params=pltpu.CompilerParams(vmem_limit_bytes=VMEM),
        cost_estimate=pl.CostEstimate(
            flops=12 * tokens * cols,
            transcendentals=tokens * cols,
            bytes_accessed=8 * tokens * cols,
        ),
        name="conv",
    )(*inputs)


def hidden_kernel(quarter, where, *refs):
    inputs, router, gates, ups = refs[:4], refs[4], refs[5:9], refs[9:13]
    hidden, *scales = refs[13:]
    gated = raised = None
    for source, gate, up in zip(inputs, gates, ups):
        rows = source[:, :quarter]
        one, two = dot(rows, gate[0]), dot(rows, up[0])
        gated = one if gated is None else gated + one
        raised = two if raised is None else raised + two
    hidden[...] = (jax.nn.silu(gated) * raised).astype(BF16)

    if not scales:
        return

    @pl.when(pl.program_id(0) == 0)
    def _():
        core, owner = where[0], where[1]
        logits = None
        for number, source in enumerate(inputs):
            block = 2 * core + number if number < 2 else 2 * (1 - core) + number - 2
            lanes = pl.ds(pl.multiple_of(block * quarter, LANES), quarter)
            term = dot_t(source[:, :quarter], router[:, lanes])
            logits = term if logits is None else logits + term
        lane = lax.broadcasted_iota(jnp.int32, logits.shape, 1)
        ids = inputs[1][:, quarter:].astype(jnp.int32)
        ids_a, ids_b = ids[:, 0:1], ids[:, 1:2]
        chosen_a = jnp.sum(jnp.where(lane == ids_a, logits, 0.0), axis=1, keepdims=True)
        chosen_b = jnp.sum(jnp.where(lane == ids_b, logits, 0.0), axis=1, keepdims=True)
        weight = jax.nn.sigmoid(chosen_a - chosen_b)
        mixed = jnp.where(ids_a == owner, weight, 0.0) + jnp.where(
            ids_b == owner, 1.0 - weight, 0.0
        )
        scales[0][...] = jnp.broadcast_to(mixed, scales[0].shape)


def hidden_units(where, inputs, router, w_gate, w_up, offset, units):
    rows, quarter = inputs[0].shape
    width = w_gate.shape[1]
    tile = math.gcd(offset, units, 256)
    base = offset // tile
    count = 1 if offset else 2

    def spec(number):
        def place(i, where):
            return 0, 2 * where[0] + number if number < 2 else 2 - 2 * where[0] + number - 2, base + i

        return pl.BlockSpec((1, quarter, tile), place)

    specs = [spec(number) for number in range(4)]
    return pl.pallas_call(
        functools.partial(hidden_kernel, quarter),
        grid_spec=pltpu.PrefetchScalarGridSpec(
            num_scalar_prefetch=1,
            grid=(units // tile,),
            in_specs=[whole(array) for array in (*inputs, router)] + specs + specs,
            out_specs=[
                pl.BlockSpec((rows, tile), lambda i, where: (0, i)),
                pl.BlockSpec((rows, LANES), lambda i, where: (0, 0)),
            ][:count],
        ),
        out_shape=[
            jax.ShapeDtypeStruct((rows, units), BF16),
            jax.ShapeDtypeStruct((rows, LANES), F32),
        ][:count],
        compiler_params=pltpu.CompilerParams(vmem_limit_bytes=VMEM_ALL),
        cost_estimate=pl.CostEstimate(
            flops=4 * rows * width * units,
            transcendentals=rows * units,
            bytes_accessed=4 * width * units + 4 * rows * width,
        ),
        name="hidden_units",
    )(where, *inputs, router, *[w_gate] * 4, *[w_up] * 4)


def down_kernel(steps, where, hidden, scale, down, send, keep):
    value = dot(hidden[...], down[0]) * scale[:, 0:1]

    @pl.when(pl.program_id(0) < steps)
    def _():
        send[...] = value.astype(BF16)

    @pl.when(pl.program_id(0) >= steps)
    def _():
        keep[...] = value


def down_units(where, hidden, scale, w_down, final):
    rows = hidden.shape[0]
    units, width = w_down.shape[1:]
    steps = width // final // 2

    def place(i, where):
        parity = jnp.where(i < steps, 1 - where[0], where[0])
        return 0, 0, 2 * lax.rem(i, steps) + parity

    return pl.pallas_call(
        functools.partial(down_kernel, steps),
        grid_spec=pltpu.PrefetchScalarGridSpec(
            num_scalar_prefetch=1,
            grid=(2 * steps,),
            in_specs=[
                whole(hidden),
                whole(scale),
                pl.BlockSpec((1, units, final), place),
            ],
            out_specs=[
                pl.BlockSpec((rows, final), lambda i, where: (0, jnp.minimum(i, steps - 1))),
                pl.BlockSpec((rows, final), lambda i, where: (0, jnp.maximum(i - steps, 0))),
            ],
        ),
        out_shape=[
            jax.ShapeDtypeStruct((rows, width // 2), BF16),
            jax.ShapeDtypeStruct((rows, width // 2), F32),
        ],
        compiler_params=pltpu.CompilerParams(vmem_limit_bytes=VMEM_ALL),
        cost_estimate=pl.CostEstimate(
            flops=2 * rows * width * units,
            transcendentals=0,
            bytes_accessed=2 * width * units + 2 * rows * (units + width),
        ),
        name="down_units",
    )(where, hidden, scale, w_down)


def collect_kernel(places, final, where, *refs):
    count = len(refs) - places - 1
    sides, outs, rows = refs[:count], refs[count:-1], refs[-1]
    offset = 0
    for pair in range(0, count, 2):
        value = sides[pair][...] + sides[pair + 1][...].astype(F32)
        rows[:, offset : offset + value.shape[1]] = value
        offset += value.shape[1]
    for mask in range(places):
        start = pl.multiple_of((where[2] ^ mask) * final, LANES)
        value = rows[:, pl.ds(start, final)]
        outs[mask][...] = value if mask == 0 else value.astype(BF16)


def collect(where, sides, final, places):
    rows = sides[0].shape[0]
    vmem = pl.BlockSpec(memory_space=pltpu.VMEM)
    return pl.pallas_call(
        functools.partial(collect_kernel, places, final),
        in_specs=[SMEM_SPEC] + [vmem] * len(sides),
        out_specs=[vmem] * places,
        out_shape=[jax.ShapeDtypeStruct((rows, final), F32)]
        + [jax.ShapeDtypeStruct((rows, final), BF16)] * (places - 1),
        scratch_shapes=[pltpu.VMEM((rows, places * final), F32)],
        compiler_params=pltpu.CompilerParams(vmem_limit_bytes=VMEM),
        name="collect",
    )(where, *sides)


def body(
    mamba_in,
    conv_state,
    in_weight,
    conv_kernel,
    conv_bias,
    moe_in,
    router,
    expert_ids,
    w_gate,
    w_up,
    w_down,
):
    tokens, width = mamba_in.shape[1:]
    channels = in_weight.shape[1]
    dp = lax.axis_size("dp")
    owners = lax.axis_size("expert")
    half = dp // 2
    me = lax.axis_index("dp")
    mine = lax.axis_index("expert")
    core = me & 1
    side = jnp.where(me >= half, 1, 0)
    local = me & (half - 1)
    place = me >> 1
    final = width // dp
    moe_rows = moe_in.shape[0]
    split = width // 2
    quarter = split // 2
    features = width // 2
    share = tokens // owners
    pieces = [channels * number // sum(CHUNKS) for number in CHUNKS]
    starts = [sum(pieces[:number]) for number in range(len(pieces))]
    where = jnp.stack([core, mine, place])
    spot = jnp.stack([local, side])
    columns = range(2, owners, 2)

    piece_out = lax.dynamic_slice(
        mamba_in, (0, mine * share, (1 - side) * features), (1, share, features)
    )[0]
    piece = xor_send(piece_out, half)

    moe_in = after(moe_in, piece_out)
    left = lax.dynamic_slice(moe_in, (0, core * split), (moe_rows, quarter))
    right = lax.dynamic_slice(moe_in, (0, core * split + quarter), (moe_rows, quarter))
    names = jnp.pad(expert_ids.astype(BF16), ((0, 0), (0, LANES - expert_ids.shape[1])))
    right = jnp.concatenate([right, names], axis=1)
    paired = xor_send(in_weight, 1)
    weights, arrived = [], []
    for start, cols in zip(starts, pieces):
        block = in_weight[:, start : start + cols]
        if len(arrived) == 1:
            block = after(block, *arrived[0], piece)
        entry, direct = [in_weight, paired], []
        for mask in range(2, half, 2):
            direct.append(xor_send(block, mask))
            entry += [direct[-1], xor_send(direct[-1], 1)]
        weights.append(entry)
        arrived.append(direct)

    lefts = {0: left, 1: owner_send(left, 1)}
    rights = {0: right}
    for mask in columns:
        rights[mask] = owner_send(right, mask)
    both = jnp.concatenate([lefts[0], lefts[1]], axis=0)
    for mask in columns:
        got = owner_send(both, mask)
        lefts[mask], lefts[mask + 1] = got[:moe_rows], got[moe_rows:]
    both = jnp.concatenate([rights[mask] for mask in range(0, owners, 2)], axis=0)
    got = owner_send(both, 1)
    for mask in range(0, owners, 2):
        rights[mask + 1] = got[mask // 2 * moe_rows : (mask // 2 + 1) * moe_rows]
    fars = [piece, owner_send(piece, 1)]
    both = jnp.concatenate(fars, axis=0)
    for mask in columns:
        fars.append(owner_send(both, mask))

    lefts = jnp.concatenate([lefts[mask] for mask in range(owners)], axis=0)
    lefts = after(lefts, fars[1], *arrived[0], *arrived[1])
    rights = jnp.concatenate([rights[mask] for mask in range(owners)], axis=0)
    inputs = [lefts, rights, xor_send(lefts, 1), xor_send(rights[:, :quarter], 1)]

    def product(chunk, *earlier):
        own, out = half_product(
            spot, mamba_in, [after(fars[0], *earlier), *fars[1:]], weights[chunk], starts[chunk], pieces[chunk]
        )
        return own, out, xor_send(out, half)

    def convolve(chunk, own, come, before):
        return conv(
            where,
            owners,
            own,
            come,
            conv_state,
            conv_kernel,
            conv_bias[None],
            starts[chunk],
            channels,
            before,
        )

    inputs[0] = after(inputs[0], paired)
    hidden, scale = hidden_units(where, inputs, router.T, w_gate, w_up, 0, w_gate.shape[2])
    own_0, out_0, come_0 = product(0, hidden, *weights[1][3::2])
    hidden = after(hidden, out_0, *arrived[2])
    send, keep = down_units(where, hidden, scale, w_down, final)
    own_1, out_1, come_1 = product(1, keep, come_0)
    taken = xor_send(after(send, out_1), 1)
    own_2, out_2, come_2 = product(2, out_1)
    taken = after(taken, out_2)
    total = (keep + taken.astype(F32)).reshape(owners, moe_rows, split)
    left, right = total[:, :, :quarter], total[:, :, quarter:]
    got = owner_send(jnp.concatenate([left[m] for m in range(1, owners, 2)], 0).astype(BF16), 1)
    got = got.reshape(owners // 2, moe_rows, quarter)
    left = {mask: left[mask] + got[mask // 2].astype(F32) for mask in range(0, owners, 2)}
    firsts, seconds = right[0], right[1]
    for mask in columns:
        got = owner_send(right[mask : mask + 2].reshape(-1, quarter).astype(BF16), mask)
        firsts = firsts + got[:moe_rows].astype(F32)
        seconds = seconds + got[moe_rows:].astype(F32)
    conv_out = convolve(0, after(own_0, firsts), come_0, None)
    lefts = left[0]
    for mask in columns:
        come = owner_send(left[mask].astype(BF16), mask)
        if mask != columns[-1]:
            lefts = lefts + come.astype(F32)
    sides = [lefts, come, firsts, owner_send(seconds.astype(BF16), 1)]
    sides[0] = after(sides[0], come_2)
    answer, *outs = collect(where, sides, final, half)
    for mask, out in enumerate(outs, 1):
        answer = answer + xor_send(out, 2 * mask).astype(F32)
    conv_out = convolve(1, own_1, come_1, conv_out)
    conv_out = convolve(2, own_2, come_2, conv_out)
    return conv_out, answer.astype(BF16)


def solution(mesh):
    in_specs = (
        P("dp", None, None),
        P("dp", None, "expert"),
        P("dp", "expert"),
        P(None, "expert"),
        P("expert"),
        P("expert", None),
        P(),
        P("expert", None),
        P("expert", None, "dp"),
        P("expert", None, "dp"),
        P("expert", "dp", None),
    )
    out_specs = (P("dp", None, "expert"), P("expert", "dp"))
    return jax.shard_map(body, mesh=mesh, in_specs=in_specs, out_specs=out_specs, check_vma=False)
```

```python
import functools
import math

import jax
import jax.numpy as jnp
from jax import lax
from jax.experimental import pallas as pl
from jax.experimental.pallas import tpu as pltpu
from jax.sharding import PartitionSpec as P

F32 = jnp.float32
BF16 = jnp.bfloat16
LANES = 128
VMEM = 24 << 20
VMEM_ALL = 56 << 20
SMEM_SPEC = pl.BlockSpec(memory_space=pltpu.SMEM)
CHUNKS = (1, 1, 2)


def xor_send(value, mask):
    pairs = [(i, i ^ mask) for i in range(lax.axis_size("dp"))]
    return lax.ppermute(value, "dp", pairs)


def owner_send(value, mask):
    pairs = [(i, i ^ mask) for i in range(lax.axis_size("expert"))]
    return lax.ppermute(value, "expert", pairs)


def after(value, *earlier):
    return lax.optimization_barrier((value, *earlier))[0]


def dot(left, right):
    return jnp.dot(left, right, preferred_element_type=F32)


def dot_t(left, right):
    return lax.dot_general(left, right, (((1,), (1,)), ((), ())), preferred_element_type=F32)


def whole(array):
    return pl.BlockSpec(array.shape, lambda *_: (0,) * array.ndim)


def tile_of(size, tile):
    return tile if size % tile == 0 else size


def half_product_kernel(blocks, depth, pieces, where, window, *refs):
    fars, weights = refs[:pieces], refs[pieces : pieces + blocks]
    near_out, far_out, rows = refs[pieces + blocks :]
    tokens = window.shape[1]

    @pl.when(pl.program_id(0) == 0)
    def _():
        for mask in range(blocks):
            source = pl.ds(pl.multiple_of((where[0] ^ mask) * depth, LANES), depth)
            lanes = slice(mask * depth, (mask + 1) * depth)
            rows[:tokens, lanes] = window[0, :, source]
            first = tokens
            for far in fars:
                rows[first : first + far.shape[0], lanes] = far[:, source]
                first += far.shape[0]

    total = None
    for mask in range(blocks):
        term = dot(rows[:, mask * depth : (mask + 1) * depth], weights[mask][...])
        total = term if mask == 0 else total + term
    near_out[...] = total[:tokens]
    far_out[...] = total[tokens:].astype(BF16)


def half_product(where, window, fars, weights, offset, cols):
    tokens, features = window.shape[1], fars[0].shape[1]
    depth = weights[0].shape[0]
    tile = math.gcd(offset, cols, 512)
    base = offset // tile

    def spec(weight):
        first = base if weight.shape[1] != cols else 0
        return pl.BlockSpec((depth, tile), lambda i, where: (0, first + i))

    return pl.pallas_call(
        functools.partial(half_product_kernel, len(weights), depth, len(fars)),
        grid_spec=pltpu.PrefetchScalarGridSpec(
            num_scalar_prefetch=1,
            grid=(cols // tile,),
            in_specs=[pl.BlockSpec((1, tokens, features), lambda i, where: (0, 0, where[1]))]
            + [whole(far) for far in fars]
            + [spec(weight) for weight in weights],
            out_specs=[pl.BlockSpec((tokens, tile), lambda i, where: (0, i))] * 2,
            scratch_shapes=[pltpu.VMEM((2 * tokens, features), BF16)],
        ),
        out_shape=[
            jax.ShapeDtypeStruct((tokens, cols), F32),
            jax.ShapeDtypeStruct((tokens, cols), BF16),
        ],
        compiler_params=pltpu.CompilerParams(vmem_limit_bytes=VMEM),
        cost_estimate=pl.CostEstimate(
            flops=4 * tokens * features * cols,
            transcendentals=0,
            bytes_accessed=2 * features * (2 * tokens + cols) + 6 * tokens * cols,
        ),
        name="half_product",
    )(where, window, *fars, *weights)


def conv_kernel_body(pad, pieces, where, own, back, state, taps, bias, *refs):
    out, rows = refs[-2:]
    tokens = own.shape[0]
    count = taps.shape[0]
    rows[pad - (count - 1) : pad, :] = state[0].astype(F32)
    share = tokens // pieces
    for mask in range(pieces):
        start = pl.multiple_of((where[1] ^ mask) * share, 8)
        piece = back[mask * share : (mask + 1) * share, :].astype(F32)
        value = (own[pl.ds(start, share), :] + piece).astype(BF16).astype(F32)
        rows[pl.ds(pl.multiple_of(pad + start, 8), share), :] = value
    summed = bias[...]
    for tap in range(count):
        first = pad - (count - 1) + tap
        summed = summed + rows[first : first + tokens, :] * taps[tap : tap + 1, :]
    out[0] = jax.nn.silu(summed).astype(BF16)


def conv(where, pieces, own, back, state, taps, bias, offset, channels, earlier):
    tokens, cols = own.shape
    tile = math.gcd(offset, cols, 512)
    base = offset // tile
    count = taps.shape[0]
    pad = 8
    inputs = [where, own, back, state, taps, bias]
    in_specs = [
        SMEM_SPEC,
        pl.BlockSpec((tokens, tile), lambda i: (0, i)),
        pl.BlockSpec((tokens, tile), lambda i: (0, i)),
        pl.BlockSpec((1, count - 1, tile), lambda i: (0, 0, base + i)),
        pl.BlockSpec((count, tile), lambda i: (0, base + i)),
        pl.BlockSpec((1, tile), lambda i: (0, base + i)),
    ]
    aliases = {}
    if earlier is not None:
        inputs.append(earlier)
        in_specs.append(pl.BlockSpec(memory_space=pl.ANY))
        aliases = {6: 0}
    return pl.pallas_call(
        functools.partial(conv_kernel_body, pad, pieces),
        grid=(cols // tile,),
        in_specs=in_specs,
        out_specs=pl.BlockSpec((1, tokens, tile), lambda i: (0, 0, base + i)),
        out_shape=jax.ShapeDtypeStruct((1, tokens, channels), BF16),
        scratch_shapes=[pltpu.VMEM((pad + tokens, tile), F32)],
        input_output_aliases=aliases,
        compiler_params=pltpu.CompilerParams(vmem_limit_bytes=VMEM),
        cost_estimate=pl.CostEstimate(
            flops=12 * tokens * cols,
            transcendentals=tokens * cols,
            bytes_accessed=8 * tokens * cols,
        ),
        name="conv",
    )(*inputs)


def hidden_kernel(quarter, where, *refs):
    inputs, router, gates, ups = refs[:4], refs[4], refs[5:9], refs[9:13]
    hidden, *scales = refs[13:]
    gated = raised = None
    for source, gate, up in zip(inputs, gates, ups):
        rows = source[:, :quarter]
        one, two = dot(rows, gate[0]), dot(rows, up[0])
        gated = one if gated is None else gated + one
        raised = two if raised is None else raised + two
    hidden[...] = (jax.nn.silu(gated) * raised).astype(BF16)

    if not scales:
        return

    @pl.when(pl.program_id(0) == 0)
    def _():
        core, owner = where[0], where[1]
        logits = None
        for number, source in enumerate(inputs):
            block = 2 * core + number if number < 2 else 2 * (1 - core) + number - 2
            lanes = pl.ds(pl.multiple_of(block * quarter, LANES), quarter)
            term = dot_t(source[:, :quarter], router[:, lanes])
            logits = term if logits is None else logits + term
        lane = lax.broadcasted_iota(jnp.int32, logits.shape, 1)
        ids = inputs[1][:, quarter:].astype(jnp.int32)
        ids_a, ids_b = ids[:, 0:1], ids[:, 1:2]
        chosen_a = jnp.sum(jnp.where(lane == ids_a, logits, 0.0), axis=1, keepdims=True)
        chosen_b = jnp.sum(jnp.where(lane == ids_b, logits, 0.0), axis=1, keepdims=True)
        weight = jax.nn.sigmoid(chosen_a - chosen_b)
        mixed = jnp.where(ids_a == owner, weight, 0.0) + jnp.where(
            ids_b == owner, 1.0 - weight, 0.0
        )
        scales[0][...] = jnp.broadcast_to(mixed, scales[0].shape)


def hidden_units(where, inputs, router, w_gate, w_up, offset, units):
    rows, quarter = inputs[0].shape
    width = w_gate.shape[1]
    tile = math.gcd(offset, units, 256)
    base = offset // tile
    count = 1 if offset else 2

    def spec(number):
        def place(i, where):
            return 0, 2 * where[0] + number if number < 2 else 2 - 2 * where[0] + number - 2, base + i

        return pl.BlockSpec((1, quarter, tile), place)

    specs = [spec(number) for number in range(4)]
    return pl.pallas_call(
        functools.partial(hidden_kernel, quarter),
        grid_spec=pltpu.PrefetchScalarGridSpec(
            num_scalar_prefetch=1,
            grid=(units // tile,),
            in_specs=[whole(array) for array in (*inputs, router)] + specs + specs,
            out_specs=[
                pl.BlockSpec((rows, tile), lambda i, where: (0, i)),
                pl.BlockSpec((rows, LANES), lambda i, where: (0, 0)),
            ][:count],
        ),
        out_shape=[
            jax.ShapeDtypeStruct((rows, units), BF16),
            jax.ShapeDtypeStruct((rows, LANES), F32),
        ][:count],
        compiler_params=pltpu.CompilerParams(vmem_limit_bytes=VMEM_ALL),
        cost_estimate=pl.CostEstimate(
            flops=4 * rows * width * units,
            transcendentals=rows * units,
            bytes_accessed=4 * width * units + 4 * rows * width,
        ),
        name="hidden_units",
    )(where, *inputs, router, *[w_gate] * 4, *[w_up] * 4)


def down_kernel(steps, where, hidden, scale, down, send, keep):
    value = dot(hidden[...], down[0]) * scale[:, 0:1]

    @pl.when(pl.program_id(0) < steps)
    def _():
        send[...] = value.astype(BF16)

    @pl.when(pl.program_id(0) >= steps)
    def _():
        keep[...] = value


def down_units(where, hidden, scale, w_down, final):
    rows = hidden.shape[0]
    units, width = w_down.shape[1:]
    steps = width // final // 2

    def place(i, where):
        parity = jnp.where(i < steps, 1 - where[0], where[0])
        return 0, 0, 2 * lax.rem(i, steps) + parity

    return pl.pallas_call(
        functools.partial(down_kernel, steps),
        grid_spec=pltpu.PrefetchScalarGridSpec(
            num_scalar_prefetch=1,
            grid=(2 * steps,),
            in_specs=[
                whole(hidden),
                whole(scale),
                pl.BlockSpec((1, units, final), place),
            ],
            out_specs=[
                pl.BlockSpec((rows, final), lambda i, where: (0, jnp.minimum(i, steps - 1))),
                pl.BlockSpec((rows, final), lambda i, where: (0, jnp.maximum(i - steps, 0))),
            ],
        ),
        out_shape=[
            jax.ShapeDtypeStruct((rows, width // 2), BF16),
            jax.ShapeDtypeStruct((rows, width // 2), F32),
        ],
        compiler_params=pltpu.CompilerParams(vmem_limit_bytes=VMEM_ALL),
        cost_estimate=pl.CostEstimate(
            flops=2 * rows * width * units,
            transcendentals=0,
            bytes_accessed=2 * width * units + 2 * rows * (units + width),
        ),
        name="down_units",
    )(where, hidden, scale, w_down)


def collect_kernel(places, final, where, *refs):
    count = len(refs) - places - 1
    sides, outs, rows = refs[:count], refs[count:-1], refs[-1]
    offset = 0
    for pair in range(0, count, 2):
        value = sides[pair][...] + sides[pair + 1][...].astype(F32)
        rows[:, offset : offset + value.shape[1]] = value
        offset += value.shape[1]
    for mask in range(places):
        start = pl.multiple_of((where[2] ^ mask) * final, LANES)
        value = rows[:, pl.ds(start, final)]
        outs[mask][...] = value if mask == 0 else value.astype(BF16)


def collect(where, sides, final, places):
    rows = sides[0].shape[0]
    vmem = pl.BlockSpec(memory_space=pltpu.VMEM)
    return pl.pallas_call(
        functools.partial(collect_kernel, places, final),
        in_specs=[SMEM_SPEC] + [vmem] * len(sides),
        out_specs=[vmem] * places,
        out_shape=[jax.ShapeDtypeStruct((rows, final), F32)]
        + [jax.ShapeDtypeStruct((rows, final), BF16)] * (places - 1),
        scratch_shapes=[pltpu.VMEM((rows, places * final), F32)],
        compiler_params=pltpu.CompilerParams(vmem_limit_bytes=VMEM),
        name="collect",
    )(where, *sides)


def body(
    mamba_in,
    conv_state,
    in_weight,
    conv_kernel,
    conv_bias,
    moe_in,
    router,
    expert_ids,
    w_gate,
    w_up,
    w_down,
):
    tokens, width = mamba_in.shape[1:]
    channels = in_weight.shape[1]
    dp = lax.axis_size("dp")
    owners = lax.axis_size("expert")
    half = dp // 2
    me = lax.axis_index("dp")
    mine = lax.axis_index("expert")
    core = me & 1
    side = jnp.where(me >= half, 1, 0)
    local = me & (half - 1)
    place = me >> 1
    final = width // dp
    moe_rows = moe_in.shape[0]
    split = width // 2
    quarter = split // 2
    features = width // 2
    share = tokens // owners
    pieces = [channels * number // sum(CHUNKS) for number in CHUNKS]
    starts = [sum(pieces[:number]) for number in range(len(pieces))]
    where = jnp.stack([core, mine, place])
    spot = jnp.stack([local, side])
    columns = range(2, owners, 2)

    piece_out = lax.dynamic_slice(
        mamba_in, (0, mine * share, (1 - side) * features), (1, share, features)
    )[0]
    piece = xor_send(piece_out, half)

    moe_in = after(moe_in, piece_out)
    left = lax.dynamic_slice(moe_in, (0, core * split), (moe_rows, quarter))
    right = lax.dynamic_slice(moe_in, (0, core * split + quarter), (moe_rows, quarter))
    names = jnp.pad(expert_ids.astype(BF16), ((0, 0), (0, LANES - expert_ids.shape[1])))
    right = jnp.concatenate([right, names], axis=1)
    paired = xor_send(in_weight, 1)
    weights, arrived = [], []
    for start, cols in zip(starts, pieces):
        block = in_weight[:, start : start + cols]
        if len(arrived) == 1:
            block = after(block, *arrived[0], piece)
        entry, direct = [in_weight, paired], []
        for mask in range(2, half, 2):
            direct.append(xor_send(block, mask))
            if len(arrived) < 2:
                entry += [direct[-1], xor_send(direct[-1], 1)]
        weights.append(entry)
        arrived.append(direct)

    lefts = {0: left, 1: owner_send(left, 1)}
    rights = {0: right}
    for mask in columns:
        rights[mask] = owner_send(right, mask)
    both = jnp.concatenate([lefts[0], lefts[1]], axis=0)
    for mask in columns:
        got = owner_send(both, mask)
        lefts[mask], lefts[mask + 1] = got[:moe_rows], got[moe_rows:]
    both = jnp.concatenate([rights[mask] for mask in range(0, owners, 2)], axis=0)
    got = owner_send(both, 1)
    for mask in range(0, owners, 2):
        rights[mask + 1] = got[mask // 2 * moe_rows : (mask // 2 + 1) * moe_rows]
    fars = [piece, owner_send(piece, 1)]
    both = jnp.concatenate(fars, axis=0)
    for mask in columns:
        fars.append(owner_send(both, mask))

    lefts = jnp.concatenate([lefts[mask] for mask in range(owners)], axis=0)
    lefts = after(lefts, fars[1], *arrived[0], *arrived[1])
    rights = jnp.concatenate([rights[mask] for mask in range(owners)], axis=0)
    inputs = [lefts, rights, xor_send(lefts, 1), xor_send(rights[:, :quarter], 1)]

    def product(chunk, *earlier):
        own, out = half_product(
            spot, mamba_in, [after(fars[0], *earlier), *fars[1:]], weights[chunk], starts[chunk], pieces[chunk]
        )
        return own, out, xor_send(out, half)

    def convolve(chunk, own, come, before):
        return conv(
            where,
            owners,
            own,
            come,
            conv_state,
            conv_kernel,
            conv_bias[None],
            starts[chunk],
            channels,
            before,
        )

    inputs[0] = after(inputs[0], paired)
    hidden, scale = hidden_units(where, inputs, router.T, w_gate, w_up, 0, w_gate.shape[2])
    own_0, out_0, come_0 = product(0, hidden, *weights[1][3::2])
    hidden = after(hidden, out_0)
    for block in arrived[2]:
        weights[2] += [block, xor_send(after(block, hidden), 1)]
    send, keep = down_units(where, hidden, scale, w_down, final)
    own_1, out_1, come_1 = product(1, keep, come_0, *weights[2][3::2])
    taken = xor_send(after(send, out_1), 1)
    own_2, out_2, come_2 = product(2, out_1)
    taken = after(taken, out_2)
    total = (keep + taken.astype(F32)).reshape(owners, moe_rows, split)
    left, right = total[:, :, :quarter], total[:, :, quarter:]
    got = owner_send(jnp.concatenate([left[m] for m in range(1, owners, 2)], 0).astype(BF16), 1)
    conv_out = convolve(0, after(own_0, out_2), come_0, None)
    got = after(got, conv_out).reshape(owners // 2, moe_rows, quarter)
    left = {mask: left[mask] + got[mask // 2].astype(F32) for mask in range(0, owners, 2)}
    firsts, seconds = right[0], right[1]
    for mask in columns:
        got = owner_send(right[mask : mask + 2].reshape(-1, quarter).astype(BF16), mask)
        firsts = firsts + got[:moe_rows].astype(F32)
        seconds = seconds + got[moe_rows:].astype(F32)
    lefts = left[0]
    for mask in columns:
        come = owner_send(left[mask].astype(BF16), mask)
        if mask != columns[-1]:
            lefts = lefts + come.astype(F32)
    sides = [lefts, come, firsts, owner_send(seconds.astype(BF16), 1)]
    sides[0] = after(sides[0], come_2)
    answer, *outs = collect(where, sides, final, half)
    for mask, out in enumerate(outs, 1):
        answer = answer + xor_send(out, 2 * mask).astype(F32)
    conv_out = convolve(2, own_2, come_2, conv_out)
    conv_out = convolve(1, own_1, come_1, conv_out)
    return conv_out, answer.astype(BF16)


def solution(mesh):
    in_specs = (
        P("dp", None, None),
        P("dp", None, "expert"),
        P("dp", "expert"),
        P(None, "expert"),
        P("expert"),
        P("expert", None),
        P(),
        P("expert", None),
        P("expert", None, "dp"),
        P("expert", None, "dp"),
        P("expert", "dp", None),
    )
    out_specs = (P("dp", None, "expert"), P("expert", "dp"))
    return jax.shard_map(body, mesh=mesh, in_specs=in_specs, out_specs=out_specs, check_vma=False)
```

```python
import functools
import math

import jax
import jax.numpy as jnp
from jax import lax
from jax.experimental import pallas as pl
from jax.experimental.pallas import tpu as pltpu
from jax.sharding import PartitionSpec as P

F32 = jnp.float32
BF16 = jnp.bfloat16
LANES = 128
VMEM = 24 << 20
VMEM_ALL = 56 << 20
SMEM_SPEC = pl.BlockSpec(memory_space=pltpu.SMEM)
CHUNKS = (3, 1, 4)


def xor_send(value, mask):
    pairs = [(i, i ^ mask) for i in range(lax.axis_size("dp"))]
    return lax.ppermute(value, "dp", pairs)


def owner_send(value, mask):
    pairs = [(i, i ^ mask) for i in range(lax.axis_size("expert"))]
    return lax.ppermute(value, "expert", pairs)


def after(value, *earlier):
    return lax.optimization_barrier((value, *earlier))[0]


def dot(left, right):
    return jnp.dot(left, right, preferred_element_type=F32)


def dot_t(left, right):
    return lax.dot_general(left, right, (((1,), (1,)), ((), ())), preferred_element_type=F32)


def whole(array):
    return pl.BlockSpec(array.shape, lambda *_: (0,) * array.ndim)


def tile_of(size, tile):
    return tile if size % tile == 0 else size


def half_product_kernel(blocks, depth, pieces, where, window, *refs):
    fars, weights = refs[:pieces], refs[pieces : pieces + blocks]
    near_out, far_out, rows = refs[pieces + blocks :]
    tokens = window.shape[1]

    @pl.when(pl.program_id(0) == 0)
    def _():
        for mask in range(blocks):
            source = pl.ds(pl.multiple_of((where[0] ^ mask) * depth, LANES), depth)
            lanes = slice(mask * depth, (mask + 1) * depth)
            rows[:tokens, lanes] = window[0, :, source]
            first = tokens
            for far in fars:
                rows[first : first + far.shape[0], lanes] = far[:, source]
                first += far.shape[0]

    total = None
    for mask in range(blocks):
        term = dot(rows[:, mask * depth : (mask + 1) * depth], weights[mask][...])
        total = term if mask == 0 else total + term
    near_out[...] = total[:tokens]
    far_out[...] = total[tokens:].astype(BF16)


def half_product(where, window, fars, weights, offset, cols):
    tokens, features = window.shape[1], fars[0].shape[1]
    depth = weights[0].shape[0]
    tile = math.gcd(offset, cols, 512)
    base = offset // tile

    def spec(weight):
        first = base if weight.shape[1] != cols else 0
        return pl.BlockSpec((depth, tile), lambda i, where: (0, first + i))

    return pl.pallas_call(
        functools.partial(half_product_kernel, len(weights), depth, len(fars)),
        grid_spec=pltpu.PrefetchScalarGridSpec(
            num_scalar_prefetch=1,
            grid=(cols // tile,),
            in_specs=[pl.BlockSpec((1, tokens, features), lambda i, where: (0, 0, where[1]))]
            + [whole(far) for far in fars]
            + [spec(weight) for weight in weights],
            out_specs=[pl.BlockSpec((tokens, tile), lambda i, where: (0, i))] * 2,
            scratch_shapes=[pltpu.VMEM((2 * tokens, features), BF16)],
        ),
        out_shape=[
            jax.ShapeDtypeStruct((tokens, cols), F32),
            jax.ShapeDtypeStruct((tokens, cols), BF16),
        ],
        compiler_params=pltpu.CompilerParams(vmem_limit_bytes=VMEM),
        cost_estimate=pl.CostEstimate(
            flops=4 * tokens * features * cols,
            transcendentals=0,
            bytes_accessed=2 * features * (2 * tokens + cols) + 6 * tokens * cols,
        ),
        name="half_product",
    )(where, window, *fars, *weights)


def conv_kernel_body(pad, pieces, where, own, back, state, taps, bias, *refs):
    out, rows = refs[-2:]
    tokens = own.shape[0]
    count = taps.shape[0]
    rows[pad - (count - 1) : pad, :] = state[0].astype(F32)
    share = tokens // pieces
    for mask in range(pieces):
        start = pl.multiple_of((where[1] ^ mask) * share, 8)
        piece = back[mask * share : (mask + 1) * share, :].astype(F32)
        value = (own[pl.ds(start, share), :] + piece).astype(BF16).astype(F32)
        rows[pl.ds(pl.multiple_of(pad + start, 8), share), :] = value
    summed = bias[...]
    for tap in range(count):
        first = pad - (count - 1) + tap
        summed = summed + rows[first : first + tokens, :] * taps[tap : tap + 1, :]
    out[0] = jax.nn.silu(summed).astype(BF16)


def conv(where, pieces, own, back, state, taps, bias, offset, channels, earlier):
    tokens, cols = own.shape
    tile = math.gcd(offset, cols, 512)
    base = offset // tile
    count = taps.shape[0]
    pad = 8
    inputs = [where, own, back, state, taps, bias]
    in_specs = [
        SMEM_SPEC,
        pl.BlockSpec((tokens, tile), lambda i: (0, i)),
        pl.BlockSpec((tokens, tile), lambda i: (0, i)),
        pl.BlockSpec((1, count - 1, tile), lambda i: (0, 0, base + i)),
        pl.BlockSpec((count, tile), lambda i: (0, base + i)),
        pl.BlockSpec((1, tile), lambda i: (0, base + i)),
    ]
    aliases = {}
    if earlier is not None:
        inputs.append(earlier)
        in_specs.append(pl.BlockSpec(memory_space=pl.ANY))
        aliases = {6: 0}
    return pl.pallas_call(
        functools.partial(conv_kernel_body, pad, pieces),
        grid=(cols // tile,),
        in_specs=in_specs,
        out_specs=pl.BlockSpec((1, tokens, tile), lambda i: (0, 0, base + i)),
        out_shape=jax.ShapeDtypeStruct((1, tokens, channels), BF16),
        scratch_shapes=[pltpu.VMEM((pad + tokens, tile), F32)],
        input_output_aliases=aliases,
        compiler_params=pltpu.CompilerParams(vmem_limit_bytes=VMEM),
        cost_estimate=pl.CostEstimate(
            flops=12 * tokens * cols,
            transcendentals=tokens * cols,
            bytes_accessed=8 * tokens * cols,
        ),
        name="conv",
    )(*inputs)


def hidden_kernel(quarter, where, *refs):
    inputs, router, gates, ups = refs[:4], refs[4], refs[5:9], refs[9:13]
    hidden, *scales = refs[13:]
    gated = raised = None
    for source, gate, up in zip(inputs, gates, ups):
        rows = source[:, :quarter]
        one, two = dot(rows, gate[0]), dot(rows, up[0])
        gated = one if gated is None else gated + one
        raised = two if raised is None else raised + two
    hidden[...] = (jax.nn.silu(gated) * raised).astype(BF16)

    if not scales:
        return

    @pl.when(pl.program_id(0) == 0)
    def _():
        core, owner = where[0], where[1]
        logits = None
        for number, source in enumerate(inputs):
            block = 2 * core + number if number < 2 else 2 * (1 - core) + number - 2
            lanes = pl.ds(pl.multiple_of(block * quarter, LANES), quarter)
            term = dot_t(source[:, :quarter], router[:, lanes])
            logits = term if logits is None else logits + term
        lane = lax.broadcasted_iota(jnp.int32, logits.shape, 1)
        ids = inputs[1][:, quarter:].astype(jnp.int32)
        ids_a, ids_b = ids[:, 0:1], ids[:, 1:2]
        chosen_a = jnp.sum(jnp.where(lane == ids_a, logits, 0.0), axis=1, keepdims=True)
        chosen_b = jnp.sum(jnp.where(lane == ids_b, logits, 0.0), axis=1, keepdims=True)
        weight = jax.nn.sigmoid(chosen_a - chosen_b)
        mixed = jnp.where(ids_a == owner, weight, 0.0) + jnp.where(
            ids_b == owner, 1.0 - weight, 0.0
        )
        scales[0][...] = jnp.broadcast_to(mixed, scales[0].shape)


def hidden_units(where, inputs, router, w_gate, w_up, offset, units):
    rows, quarter = inputs[0].shape
    width = w_gate.shape[1]
    tile = math.gcd(offset, units, 256)
    base = offset // tile
    count = 1 if offset else 2

    def spec(number):
        def place(i, where):
            return 0, 2 * where[0] + number if number < 2 else 2 - 2 * where[0] + number - 2, base + i

        return pl.BlockSpec((1, quarter, tile), place)

    specs = [spec(number) for number in range(4)]
    return pl.pallas_call(
        functools.partial(hidden_kernel, quarter),
        grid_spec=pltpu.PrefetchScalarGridSpec(
            num_scalar_prefetch=1,
            grid=(units // tile,),
            in_specs=[whole(array) for array in (*inputs, router)] + specs + specs,
            out_specs=[
                pl.BlockSpec((rows, tile), lambda i, where: (0, i)),
                pl.BlockSpec((rows, LANES), lambda i, where: (0, 0)),
            ][:count],
        ),
        out_shape=[
            jax.ShapeDtypeStruct((rows, units), BF16),
            jax.ShapeDtypeStruct((rows, LANES), F32),
        ][:count],
        compiler_params=pltpu.CompilerParams(vmem_limit_bytes=VMEM_ALL),
        cost_estimate=pl.CostEstimate(
            flops=4 * rows * width * units,
            transcendentals=rows * units,
            bytes_accessed=4 * width * units + 4 * rows * width,
        ),
        name="hidden_units",
    )(where, *inputs, router, *[w_gate] * 4, *[w_up] * 4)


def down_kernel(steps, where, hidden, scale, down, send, keep):
    value = dot(hidden[...], down[0]) * scale[:, 0:1]

    @pl.when(pl.program_id(0) < steps)
    def _():
        send[...] = value.astype(BF16)

    @pl.when(pl.program_id(0) >= steps)
    def _():
        keep[...] = value


def down_units(where, hidden, scale, w_down, final):
    rows = hidden.shape[0]
    units, width = w_down.shape[1:]
    steps = width // final // 2

    def place(i, where):
        parity = jnp.where(i < steps, 1 - where[0], where[0])
        return 0, 0, 2 * lax.rem(i, steps) + parity

    return pl.pallas_call(
        functools.partial(down_kernel, steps),
        grid_spec=pltpu.PrefetchScalarGridSpec(
            num_scalar_prefetch=1,
            grid=(2 * steps,),
            in_specs=[
                whole(hidden),
                whole(scale),
                pl.BlockSpec((1, units, final), place),
            ],
            out_specs=[
                pl.BlockSpec((rows, final), lambda i, where: (0, jnp.minimum(i, steps - 1))),
                pl.BlockSpec((rows, final), lambda i, where: (0, jnp.maximum(i - steps, 0))),
            ],
        ),
        out_shape=[
            jax.ShapeDtypeStruct((rows, width // 2), BF16),
            jax.ShapeDtypeStruct((rows, width // 2), F32),
        ],
        compiler_params=pltpu.CompilerParams(vmem_limit_bytes=VMEM_ALL),
        cost_estimate=pl.CostEstimate(
            flops=2 * rows * width * units,
            transcendentals=0,
            bytes_accessed=2 * width * units + 2 * rows * (units + width),
        ),
        name="down_units",
    )(where, hidden, scale, w_down)


def collect_kernel(places, final, where, *refs):
    count = len(refs) - places - 1
    sides, outs, rows = refs[:count], refs[count:-1], refs[-1]
    offset = 0
    for pair in range(0, count, 2):
        value = sides[pair][...] + sides[pair + 1][...].astype(F32)
        rows[:, offset : offset + value.shape[1]] = value
        offset += value.shape[1]
    for mask in range(places):
        start = pl.multiple_of((where[2] ^ mask) * final, LANES)
        value = rows[:, pl.ds(start, final)]
        outs[mask][...] = value if mask == 0 else value.astype(BF16)


def collect(where, sides, final, places):
    rows = sides[0].shape[0]
    vmem = pl.BlockSpec(memory_space=pltpu.VMEM)
    return pl.pallas_call(
        functools.partial(collect_kernel, places, final),
        in_specs=[SMEM_SPEC] + [vmem] * len(sides),
        out_specs=[vmem] * places,
        out_shape=[jax.ShapeDtypeStruct((rows, final), F32)]
        + [jax.ShapeDtypeStruct((rows, final), BF16)] * (places - 1),
        scratch_shapes=[pltpu.VMEM((rows, places * final), F32)],
        compiler_params=pltpu.CompilerParams(vmem_limit_bytes=VMEM),
        name="collect",
    )(where, *sides)


def body(
    mamba_in,
    conv_state,
    in_weight,
    conv_kernel,
    conv_bias,
    moe_in,
    router,
    expert_ids,
    w_gate,
    w_up,
    w_down,
):
    tokens, width = mamba_in.shape[1:]
    channels = in_weight.shape[1]
    dp = lax.axis_size("dp")
    owners = lax.axis_size("expert")
    half = dp // 2
    me = lax.axis_index("dp")
    mine = lax.axis_index("expert")
    core = me & 1
    side = jnp.where(me >= half, 1, 0)
    local = me & (half - 1)
    place = me >> 1
    final = width // dp
    moe_rows = moe_in.shape[0]
    split = width // 2
    quarter = split // 2
    features = width // 2
    share = tokens // owners
    pieces = [channels * number // sum(CHUNKS) for number in CHUNKS]
    starts = [sum(pieces[:number]) for number in range(len(pieces))]
    where = jnp.stack([core, mine, place])
    spot = jnp.stack([local, side])
    columns = range(2, owners, 2)

    piece_out = lax.dynamic_slice(
        mamba_in, (0, mine * share, (1 - side) * features), (1, share, features)
    )[0]
    piece = xor_send(piece_out, half)

    moe_in = after(moe_in, piece_out)
    left = lax.dynamic_slice(moe_in, (0, core * split), (moe_rows, quarter))
    right = lax.dynamic_slice(moe_in, (0, core * split + quarter), (moe_rows, quarter))
    names = jnp.pad(expert_ids.astype(BF16), ((0, 0), (0, LANES - expert_ids.shape[1])))
    right = jnp.concatenate([right, names], axis=1)
    paired = xor_send(in_weight, 1)
    weights, arrived = [], []
    for start, cols in zip(starts, pieces):
        block = in_weight[:, start : start + cols]
        if len(arrived) == 1:
            block = after(block, *arrived[0], piece)
        entry, direct = [in_weight, paired], []
        for mask in range(2, half, 2):
            direct.append(xor_send(block, mask))
            if len(arrived) < 2:
                entry += [direct[-1], xor_send(direct[-1], 1)]
        weights.append(entry)
        arrived.append(direct)

    lefts = {0: left, 1: owner_send(left, 1)}
    rights = {0: right}
    for mask in columns:
        rights[mask] = owner_send(right, mask)
    both = jnp.concatenate([lefts[0], lefts[1]], axis=0)
    for mask in columns:
        got = owner_send(both, mask)
        lefts[mask], lefts[mask + 1] = got[:moe_rows], got[moe_rows:]
    both = jnp.concatenate([rights[mask] for mask in range(0, owners, 2)], axis=0)
    got = owner_send(both, 1)
    for mask in range(0, owners, 2):
        rights[mask + 1] = got[mask // 2 * moe_rows : (mask // 2 + 1) * moe_rows]
    fars = [piece, owner_send(piece, 1)]
    both = jnp.concatenate(fars, axis=0)
    for mask in columns:
        fars.append(owner_send(both, mask))

    lefts = jnp.concatenate([lefts[mask] for mask in range(owners)], axis=0)
    lefts = after(lefts, fars[1], *arrived[0], *arrived[1])
    rights = jnp.concatenate([rights[mask] for mask in range(owners)], axis=0)
    inputs = [lefts, rights, xor_send(lefts, 1), xor_send(rights[:, :quarter], 1)]

    def product(chunk, *earlier):
        own, out = half_product(
            spot, mamba_in, [after(fars[0], *earlier), *fars[1:]], weights[chunk], starts[chunk], pieces[chunk]
        )
        return own, out, xor_send(out, half)

    def convolve(chunk, own, come, before):
        return conv(
            where,
            owners,
            own,
            come,
            conv_state,
            conv_kernel,
            conv_bias[None],
            starts[chunk],
            channels,
            before,
        )

    inputs[0] = after(inputs[0], paired)
    hidden, scale = hidden_units(where, inputs, router.T, w_gate, w_up, 0, w_gate.shape[2])
    own_0, out_0, come_0 = product(0, hidden, *weights[1][3::2])
    hidden = after(hidden, out_0)
    for block in arrived[2]:
        weights[2] += [block, xor_send(after(block, hidden), 1)]
    send, keep = down_units(where, hidden, scale, w_down, final)
    own_1, out_1, come_1 = product(1, keep, come_0, *weights[2][3::2])
    taken = xor_send(after(send, out_1), 1)
    own_2, out_2, come_2 = product(2, out_1)
    taken = after(taken, out_2)
    total = (keep + taken.astype(F32)).reshape(owners, moe_rows, split)
    left, right = total[:, :, :quarter], total[:, :, quarter:]
    got = owner_send(jnp.concatenate([left[m] for m in range(1, owners, 2)], 0).astype(BF16), 1)
    conv_out = convolve(0, after(own_0, out_2), come_0, None)
    got = after(got, conv_out).reshape(owners // 2, moe_rows, quarter)
    left = {mask: left[mask] + got[mask // 2].astype(F32) for mask in range(0, owners, 2)}
    firsts, seconds = right[0], right[1]
    for mask in columns:
        got = owner_send(right[mask : mask + 2].reshape(-1, quarter).astype(BF16), mask)
        firsts = firsts + got[:moe_rows].astype(F32)
        seconds = seconds + got[moe_rows:].astype(F32)
    lefts = left[0]
    for mask in columns:
        come = owner_send(left[mask].astype(BF16), mask)
        if mask != columns[-1]:
            lefts = lefts + come.astype(F32)
    sides = [lefts, come, firsts, owner_send(seconds.astype(BF16), 1)]
    sides[0] = after(sides[0], come_2)
    answer, *outs = collect(where, sides, final, half)
    for mask, out in enumerate(outs, 1):
        answer = answer + xor_send(out, 2 * mask).astype(F32)
    conv_out = convolve(2, own_2, come_2, conv_out)
    conv_out = convolve(1, own_1, come_1, conv_out)
    return conv_out, answer.astype(BF16)


def solution(mesh):
    in_specs = (
        P("dp", None, None),
        P("dp", None, "expert"),
        P("dp", "expert"),
        P(None, "expert"),
        P("expert"),
        P("expert", None),
        P(),
        P("expert", None),
        P("expert", None, "dp"),
        P("expert", None, "dp"),
        P("expert", "dp", None),
    )
    out_specs = (P("dp", None, "expert"), P("expert", "dp"))
    return jax.shard_map(body, mesh=mesh, in_specs=in_specs, out_specs=out_specs, check_vma=False)
```
